32 devices in a mesh: scene: 2 (over y), cam: 16 (over z, x, core).
Axes of the slice: x: 2, y: 2, z: 4, core: 2. Of those that a mesh axis runs over, the one named last changes fastest.
Arguments:
- queries: bfloat16 [32, 768, 1024], P(('scene', 'cam')), parts along dimension 0, may hold values from -32 to 32
- keys: bfloat16 [32, 768, 1024], P(('scene', 'cam')), parts along dimension 0, may hold values from -32 to 32
- values: bfloat16 [32, 768, 1024], P(('scene', 'cam')), parts along dimension 0, may hold values from -6 to 6
- residual: bfloat16 [32, 768, 1024], P(('scene', 'cam')), parts along dimension 0, may hold values from -1.5 to 1.5
- w_out: bfloat16 [1024, 1024], replicated, may hold values from -0.1875 to 0.1875
- neighbours: int32 [32, 4], P(('scene', 'cam')), parts along dimension 0, may hold values from 0 to 15, as said below
- band_start: int32 [32, 4], P(('scene', 'cam')), parts along dimension 0, may hold values from 0 to 3
- band_blocks: int32 [32, 4, 6, 2], P(('scene', 'cam')), parts along dimension 0, may hold values from 0 to 2, as said below
- band_count: int32 [32, 4, 6], P(('scene', 'cam')), parts along dimension 0, may hold values from 1 to 2, as said below
Outputs:
- output: bfloat16 [32, 768, 1024], P(('scene', 'cam')), parts along dimension 0
The draws below stay inside these ranges and needn't reach their ends.
There are 2 independent parts, one for each index of `scene`. The reference program is written for one: setup_inputs(seed, part) draws one part's arguments, and reference() takes and returns one part's arrays. A program takes and returns all parts, laid end to end along the dimension named above; an argument that names none is the same for every part. Nothing has to cross between parts.
Inputs may be any that keep to these rules, and one draw needn't show every extreme that they name: `neighbours`: row v lists the views (v + k) mod 16 for k = 1, -1, 2, -2, each once, in an order drawn for each row. `band_blocks`: each list holds 2 different numbers; entries at positions band_count or later are not read. `band_count`: query block 0 of every slot has 2.
All inputs are finite; a program needn't handle non-finite values.
Results may differ from the reference program's by a relative error of at most 0.008.
Values may be sent and summed in bfloat16 or wider, within the bound.
A program may use at most 128 MiB of HBM per device.

```python
import jax
import jax.numpy as jnp
from jax import lax

D = 1024
HEADS = 16
TOK = 768
MOST = 2
RIGS = 1
VIEWS = 16
QB = 6
WIN = 3


def drawn_pair(key):
    base_key = jax.random.fold_in(key, 17)
    query_key, key_key = jax.random.split(base_key, 2)
    query_draw = 2.0 * jnp.clip(jax.random.normal(query_key, (VIEWS, TOK, D), jnp.float32), -6.0, 6.0)
    key_draw = jnp.clip(jax.random.normal(key_key, (VIEWS, TOK, D), jnp.float32), -6.0, 6.0)
    return (query_draw.astype(jnp.bfloat16), key_draw.astype(jnp.bfloat16))


def draw_queries(key, part):
    return drawn_pair(key)[0]


def draw_keys(key, part):
    return drawn_pair(key)[1]


def draw_neighbours(key, part):
    order_key = jax.random.fold_in(key, 3)
    ranks = jax.random.randint(order_key, (VIEWS, 4), 0, 1 << 20) * 4 + jnp.arange(4, dtype=jnp.int32)[None, :]
    order = jnp.argsort(ranks, axis=1, stable=True)
    offsets = jnp.array([1, -1, 2, -2], dtype=jnp.int32)[order]
    views = jnp.arange(VIEWS, dtype=jnp.int32)[:, None]
    return ((views + offsets * RIGS + 2 * VIEWS) % VIEWS).astype(jnp.int32)


def draw_band_blocks(key, part):
    order_key = jax.random.fold_in(key, 5)
    ranks = jax.random.randint(order_key, (VIEWS, 4, QB, WIN), 0, 1 << 20) * WIN + jnp.arange(WIN, dtype=jnp.int32)
    order = jnp.argsort(ranks, axis=-1, stable=True)
    return order[..., :MOST].astype(jnp.int32)


def draw_band_count(key, part):
    level_key = jax.random.fold_in(key, 7)
    roll_key = jax.random.fold_in(key, 11)
    levels = jax.random.randint(level_key, (VIEWS, 1, 1), 1, 10)
    rolls = jax.random.randint(roll_key, (VIEWS, 4, QB), 0, 10)
    counted = jnp.where(rolls < levels, MOST, 1).astype(jnp.int32)
    return counted.at[:, :, 0].set(MOST)


def plant(values, rng, low, top_value):
    place = [jax.random.randint(jax.random.fold_in(rng, axis), (), 0, length) for axis, length in enumerate(values.shape)]
    main_axis = values.shape.index(max(values.shape))
    neighbour = place[:main_axis] + [(place[main_axis] + 1) % values.shape[main_axis]] + place[main_axis + 1:]
    return values.at[tuple(place)].set(low).at[tuple(neighbour)].set(top_value)


def shard_levels(key, dims, cuts, least, high):
    def one(dim, shards_of):
        draws = jax.random.uniform(jax.random.fold_in(jax.random.fold_in(key, 6), dim), (shards_of,), jnp.float32, least / len(cuts), high / len(cuts))
        return jnp.repeat(jnp.exp(draws), dims[dim] // shards_of).reshape((-1,) + (1,) * (len(dims) - dim - 1))

    level = one(*cuts[0])
    for cut in cuts[1:]:
        level = level * one(*cut)
    return level


def gaussian(stream_key, dims, width, reach, cuts=(), kind=jnp.bfloat16):
    values = width * jax.random.normal(stream_key, dims, jnp.float32)
    if cuts:
        values = values * shard_levels(stream_key, dims, cuts, -0.22, 0.18)
    return jnp.clip(values, -reach, reach).astype(kind)


def setup_inputs(seed: int = 0, part: int = 0) -> dict:
    key_list = jax.random.split(jax.random.key(seed), 10)
    part_keys = jax.random.split(jax.random.fold_in(key_list[9], part), 10)
    queries = draw_queries(jax.random.fold_in(jax.random.fold_in(key_list[9], part), 71), part)
    keys = draw_keys(jax.random.fold_in(jax.random.fold_in(key_list[9], part), 71), part)
    values = gaussian(part_keys[2], (VIEWS, TOK, D), 1.0, 6.0, ((0, 16),))
    residual = gaussian(part_keys[3], (VIEWS, TOK, D), 0.25, 1.5, ((0, 16),))
    w_out = gaussian(key_list[4], (D, D), D ** -0.5, 0.1875)
    neighbours = draw_neighbours(jax.random.fold_in(jax.random.fold_in(key_list[9], part), 71), part)
    band_start = plant(jax.random.randint(part_keys[6], (VIEWS, 4), 0, QB - WIN + 1), jax.random.fold_in(part_keys[6], 1), 0, QB - WIN).astype(jnp.int32)
    band_blocks = draw_band_blocks(jax.random.fold_in(jax.random.fold_in(key_list[9], part), 71), part)
    band_count = draw_band_count(jax.random.fold_in(jax.random.fold_in(key_list[9], part), 71), part)
    return dict(queries=queries, keys=keys, values=values, residual=residual, w_out=w_out, neighbours=neighbours, band_start=band_start, band_blocks=band_blocks, band_count=band_count)


def reference(queries, keys, values, residual, w_out, neighbours, band_start, band_blocks, band_count):
    cameras, tokens, model_width = queries.shape
    qblocks = band_count.shape[2]
    most_blocks = band_blocks.shape[3]
    block_len = tokens // qblocks
    head_dim = model_width // HEADS
    score_scale = 1.0 / (head_dim ** 0.5)
    key_tiles = keys.reshape(cameras, qblocks, block_len, model_width)
    value_tiles = values.reshape(cameras, qblocks, block_len, model_width)

    def one_view(view_index):
        near_cams = neighbours[view_index]
        absolute = band_start[view_index][:, None, None] + band_blocks[view_index]
        near_keys = key_tiles[near_cams[:, None, None], absolute]
        near_values = value_tiles[near_cams[:, None, None], absolute]
        near_keys = jnp.transpose(near_keys, (1, 0, 2, 3, 4)).reshape(qblocks, 4 * most_blocks * block_len, model_width)
        near_values = jnp.transpose(near_values, (1, 0, 2, 3, 4)).reshape(qblocks, 4 * most_blocks * block_len, model_width)
        all_keys = jnp.concatenate([key_tiles[view_index], near_keys], axis=1).reshape(qblocks, -1, HEADS, head_dim)
        all_values = jnp.concatenate([value_tiles[view_index], near_values], axis=1).reshape(qblocks, -1, HEADS, head_dim)
        live_slots = jnp.arange(most_blocks, dtype=jnp.int32)[None, None, :] < band_count[view_index][:, :, None]
        live_slots = jnp.repeat(jnp.transpose(live_slots, (1, 0, 2)), block_len, axis=2).reshape(qblocks, -1)
        visible = jnp.concatenate([jnp.ones((qblocks, block_len), dtype=bool), live_slots], axis=1)
        query_tiles = queries[view_index].reshape(qblocks, block_len, HEADS, head_dim)
        scores = jnp.einsum("gqhd,gkhd->ghqk", query_tiles.astype(jnp.float32), all_keys.astype(jnp.float32)) * score_scale
        scores = jnp.where(visible[:, None, None, :], scores, -jnp.inf)
        row_max = jnp.max(scores, axis=-1, keepdims=True)
        expo_scores = jnp.exp(scores - row_max)
        weights = (expo_scores / jnp.sum(expo_scores, axis=-1, keepdims=True)).astype(jnp.bfloat16)
        attended = jnp.einsum("ghqk,gkhd->gqhd", weights.astype(jnp.float32), all_values.astype(jnp.float32))
        attended = attended.astype(jnp.bfloat16).reshape(tokens, model_width)
        projected = jnp.dot(attended, w_out, preferred_element_type=jnp.float32)
        return (residual[view_index].astype(jnp.float32) + projected).astype(jnp.bfloat16)

    return lax.map(one_view, jnp.arange(cameras, dtype=jnp.int32))
```

```python
import functools
import math

import jax
import jax.numpy as jnp
from jax import lax
from jax.experimental import pallas as pl
from jax.experimental.pallas import tpu as pltpu
from jax.sharding import PartitionSpec as P

HEADS = 16
LANES = 128
ROLES = 4
HIDDEN = -1e30


def kernel(cfg, q_hbm, k_hbm, v_hbm, near_ref, start_ref, block_ref, count_ref, out_ref, *scratch):
    cameras, rigs, chunks, qblocks, most, head_dim = cfg
    relay = rigs == 1 and cameras % 4 == 0
    buffers = [scratch[r * chunks:(r + 1) * chunks] for r in range(ROLES)]
    q_ref, k_ref, v_ref, own_sem, first_send, first_recv, next_send, next_recv = scratch[ROLES * chunks:]
    part_a, part_b, part_x, part_z = range(ROLES)
    block_len = q_ref.shape[1]
    me = lax.axis_index("cam")

    def at(offset):
        return lax.rem(me + offset + 2 * cameras, cameras)

    if relay:
        column = lax.rem(me // 2, 2)
        core = lax.rem(me, 2)
        partner = me + 1 - 2 * core
        across = me + 2 - 4 * column
        z_to = at(4 - 8 * column)
        z_from = at(8 * column - 4)
        from_x = lax.rem(column + core, 2) == 0
        z_view = at(4 * column - 2)
        partner_x = partner + 2 - 4 * column
        partner_z = lax.rem(partner + 4 * column - 2 + cameras, cameras)
        b_view = jnp.where(from_x, partner_z, partner_x)
        views = (partner, b_view, across, z_view)
        peers = (partner, across, z_to, z_from)
        first = ((part_x, across), (part_a, partner))
    else:
        views = (at(rigs), at(-rigs), at(2 * rigs), at(-2 * rigs))
        peers = views
        first = (
            (part_a, views[1]), (part_b, views[0]), (part_x, views[3]), (part_z, views[2])
        )

    own_copies = [
        pltpu.make_async_copy(src, dst, own_sem.at[n])
        for n, (src, dst) in enumerate(((q_hbm, q_ref), (k_hbm, k_ref), (v_hbm, v_ref)))
    ]
    for copy in own_copies:
        copy.start()
    barrier = pltpu.get_barrier_semaphore()
    for peer in peers:
        pl.semaphore_signal(
            barrier, inc=1, device_id={"cam": peer}, device_id_type=pl.DeviceIdType.MESH
        )
    pl.semaphore_wait(barrier, len(peers))

    def first_copy(lane, g, kind):
        role, target = first[lane]
        source = (k_hbm, v_hbm)[kind]
        return pltpu.make_async_remote_copy(
            src_ref=source.at[:, :, pl.ds(g * LANES, LANES)],
            dst_ref=buffers[role][g].at[kind],
            send_sem=first_send.at[lane, g, kind],
            recv_sem=first_recv.at[lane, g, kind],
            device_id={"cam": target},
            device_id_type=pl.DeviceIdType.MESH,
        )

    def next_copy(role, g, source_role, target):
        return pltpu.make_async_remote_copy(
            src_ref=buffers[source_role][g],
            dst_ref=buffers[role][g],
            send_sem=next_send.at[role // 2, g],
            recv_sem=next_recv.at[role // 2, g],
            device_id={"cam": target},
            device_id_type=pl.DeviceIdType.MESH,
        )

    for lane in range(len(first)):
        for g in range(chunks):
            for kind in range(2):
                first_copy(lane, g, kind).start()

    def first_wait(lane, g):
        for kind in range(2):
            first_copy(lane, g, kind).wait_recv()

    slots = []
    for view in views:
        slot = jnp.int32(0)
        for s in range(1, ROLES):
            slot = jnp.where(near_ref[0, s] == view, s, slot)
        slots.append(slot)
    starts = [start_ref[0, slot] for slot in slots]

    def compute(g):
        cols = slice(g * LANES, (g + 1) * LANES)

        def one_block(b, carry):
            heads = LANES // head_dim
            q = q_ref[b, :, cols] * jnp.asarray(1.0 / math.sqrt(head_dim), jnp.bfloat16)
            lane = lax.broadcasted_iota(jnp.int32, (block_len, LANES), 1) // head_dim
            q2 = jnp.concatenate(
                [jnp.where(lane == h, q, jnp.zeros_like(q)) for h in range(heads)], axis=0
            )
            dims = (((1,), (1,)), ((), ()))
            scores = [
                lax.dot_general(q2, k_ref[b, :, cols], dims, preferred_element_type=jnp.float32)
            ]
            vals = [v_ref[b, :, cols]]
            for r in range(ROLES):
                buffer = buffers[r][g]
                key_parts, val_parts, bias = [], [], []
                live = count_ref[0, slots[r], b]
                for m in range(most):
                    near = starts[r] + block_ref[0, slots[r], b, m]
                    if m > 0:
                        near = jnp.where(m < live, near, 0)
                        bias.append(jnp.where(m < live, 0.0, HIDDEN))
                    key_parts.append(buffer[0, near])
                    val_parts.append(buffer[1, near])
                got = lax.dot_general(
                    q2,
                    jnp.concatenate(key_parts, axis=0),
                    dims,
                    preferred_element_type=jnp.float32,
                )
                pieces = [got[:, :block_len]]
                for m in range(1, most):
                    pieces.append(got[:, m * block_len:(m + 1) * block_len] + bias[m - 1])
                scores.append(jnp.concatenate(pieces, axis=1))
                vals.append(jnp.concatenate(val_parts, axis=0))
            all_scores = jnp.concatenate(scores, axis=1)
            top = jnp.max(all_scores, axis=1, keepdims=True)
            expo = jnp.exp(all_scores - top)
            total = jnp.sum(expo, axis=1, keepdims=True)
            mixed = jnp.dot(
                expo.astype(jnp.bfloat16),
                jnp.concatenate(vals, axis=0),
                preferred_element_type=jnp.float32,
            )
            mixed = mixed / total
            result = mixed[:block_len]
            for h in range(1, heads):
                result = jnp.where(lane == h, mixed[h * block_len:(h + 1) * block_len], result)
            out_ref[b, :, cols] = result.astype(out_ref.dtype)
            return carry

        lax.fori_loop(0, qblocks, one_block, 0)

    if relay:

        def z_send(g):
            return next_copy(part_z, g, part_x, z_to)

        def b_send(g, source):
            return next_copy(part_b, g, source, partner)

        def after_x(g):
            first_wait(0, g)
            z_send(g).start()

            @pl.when(from_x)
            def _():
                b_send(g, part_x).start()

        def after_z(g):
            z_send(g).wait_recv()

            @pl.when(jnp.logical_not(from_x))
            def _():
                b_send(g, part_z).start()

        def finish(g):
            first_wait(1, g)
            b_send(g, part_x).wait_recv()
            compute(g)

        for step in range(chunks):
            after_x(step)
            if step >= 1:
                after_z(step - 1)
            if step == 1:
                for copy in own_copies:
                    copy.wait()
            if step >= 2:
                finish(step - 2)
        if chunks >= 2:
            finish(chunks - 2)
        else:
            for copy in own_copies:
                copy.wait()
        after_z(chunks - 1)
        finish(chunks - 1)
        for g in range(chunks):
            z_send(g).wait_send()

            @pl.when(from_x)
            def _():
                b_send(g, part_x).wait_send()

            @pl.when(jnp.logical_not(from_x))
            def _():
                b_send(g, part_z).wait_send()
    else:
        for copy in own_copies:
            copy.wait()
        for g in range(chunks):
            for lane in range(len(first)):
                first_wait(lane, g)
            compute(g)
    for lane in range(len(first)):
        for g in range(chunks):
            for kind in range(2):
                first_copy(lane, g, kind).wait_send()


def per_device(
    queries, keys, values, residual, w_out, neighbours, band_start, band_blocks, band_count
):
    tokens, width = queries.shape[1:]
    qblocks = band_count.shape[2]
    most = band_blocks.shape[3]
    cameras = lax.axis_size("cam")
    rigs = cameras // min(32, cameras)
    chunks = width // LANES
    cfg = (cameras, rigs, chunks, qblocks, most, width // HEADS)
    lanes = 2 if rigs == 1 and cameras % 4 == 0 else 4
    dma = pltpu.SemaphoreType.DMA
    anywhere = pl.BlockSpec(memory_space=pl.ANY)
    scalars = pl.BlockSpec(memory_space=pltpu.SMEM)
    blocks = (qblocks, tokens // qblocks, width)
    attended = pl.pallas_call(
        functools.partial(kernel, cfg),
        out_shape=jax.ShapeDtypeStruct(blocks, jnp.bfloat16),
        in_specs=[anywhere] * 3 + [scalars] * 4,
        out_specs=pl.BlockSpec(memory_space=pltpu.VMEM),
        scratch_shapes=[pltpu.VMEM((2,) + blocks[:2] + (LANES,), jnp.bfloat16)] * (ROLES * chunks)
        + [pltpu.VMEM(blocks, jnp.bfloat16)] * 3
        + [
            dma((3,)),
            dma((lanes, chunks, 2)),
            dma((lanes, chunks, 2)),
            dma((2, chunks)),
            dma((2, chunks)),
        ],
        compiler_params=pltpu.CompilerParams(
            collective_id=0, has_side_effects=True, vmem_limit_bytes=48 * 1024 * 1024
        ),
        name="band_attention",
    )(*(x[0].reshape(blocks) for x in (queries, keys, values)), neighbours, band_start, band_blocks, band_count)
    result = residual[0].astype(jnp.float32) + jnp.dot(
        attended.reshape(tokens, width), w_out, preferred_element_type=jnp.float32
    )
    return result.astype(jnp.bfloat16)[None]


def solution(mesh):
    rows = ("scene", "cam")
    return jax.shard_map(
        per_device,
        mesh=mesh,
        in_specs=(
            P(rows, None, None),
            P(rows, None, None),
            P(rows, None, None),
            P(rows, None, None),
            P(),
            P(rows, None),
            P(rows, None),
            P(rows, None, None, None),
            P(rows, None, None),
        ),
        out_specs=P(rows, None, None),
        check_vma=False,
    )
```

```python
import functools
import math

import jax
import jax.numpy as jnp
from jax import lax
from jax.experimental import pallas as pl
from jax.experimental.pallas import tpu as pltpu
from jax.sharding import PartitionSpec as P

HEADS = 16
LANES = 128
ROLES = 4
HIDDEN = -1e30


def relays(cameras, rigs, qblocks):
    return rigs == 1 and cameras % 4 == 0 and qblocks % 2 == 0


def kernel(cfg, q_hbm, k_hbm, v_hbm, near_ref, start_ref, block_ref, count_ref, out_ref, *scratch):
    cameras, rigs, chunks, qblocks, most, head_dim = cfg
    relay = relays(cameras, rigs, qblocks)
    buffers = [scratch[r * chunks:(r + 1) * chunks] for r in range(ROLES)]
    q_ref, k_ref, v_ref, own_sem, first_send, first_recv, next_send, next_recv = scratch[ROLES * chunks:]
    part_a, part_b, part_x, part_z = range(ROLES)
    block_len = q_ref.shape[1]
    me = lax.axis_index("cam")

    def at(offset):
        return lax.rem(me + offset + 2 * cameras, cameras)

    if relay:
        column = lax.rem(me // 2, 2)
        core = lax.rem(me, 2)
        partner = me + 1 - 2 * core
        across = me + 2 - 4 * column
        z_to = at(4 - 8 * column)
        z_from = at(8 * column - 4)
        from_x = lax.rem(column + core, 2) == 0
        z_view = at(4 * column - 2)
        partner_x = partner + 2 - 4 * column
        partner_z = lax.rem(partner + 4 * column - 2 + cameras, cameras)
        b_view = jnp.where(from_x, partner_z, partner_x)
        views = (partner, b_view, across, z_view)
        peers = (partner, across, z_to, z_from)
        first = ((part_x, across), (part_a, partner))
    else:
        views = (at(rigs), at(-rigs), at(2 * rigs), at(-2 * rigs))
        peers = views
        first = (
            (part_a, views[1]), (part_b, views[0]), (part_x, views[3]), (part_z, views[2])
        )

    own_copies = [
        pltpu.make_async_copy(src, dst, own_sem.at[n])
        for n, (src, dst) in enumerate(((q_hbm, q_ref), (k_hbm, k_ref), (v_hbm, v_ref)))
    ]
    for copy in own_copies:
        copy.start()
    barrier = pltpu.get_barrier_semaphore()
    for peer in peers:
        pl.semaphore_signal(
            barrier, inc=1, device_id={"cam": peer}, device_id_type=pl.DeviceIdType.MESH
        )
    pl.semaphore_wait(barrier, len(peers))

    def first_copy(lane, g, kind, rows):
        role, target = first[lane]
        source = (v_hbm if isinstance(kind, int) and kind == 1 else k_hbm)
        part = kind * (qblocks // rows.size) + rows.start // rows.size
        return pltpu.make_async_remote_copy(
            src_ref=source.at[rows, :, pl.ds(g * LANES, LANES)],
            dst_ref=buffers[role][g].at[kind, rows],
            send_sem=first_send.at[lane, g, part],
            recv_sem=first_recv.at[lane, g, part],
            device_id={"cam": target},
            device_id_type=pl.DeviceIdType.MESH,
        )

    def next_copy(role, g, source_role, target, part):
        kind, rows = piece(part)
        return pltpu.make_async_remote_copy(
            src_ref=buffers[source_role][g].at[kind, rows],
            dst_ref=buffers[role][g].at[kind, rows],
            send_sem=next_send.at[role // 2, g, part],
            recv_sem=next_recv.at[role // 2, g, part],
            device_id={"cam": target},
            device_id_type=pl.DeviceIdType.MESH,
        )

    splits = qblocks // 2 if relay else 1

    def piece(part):
        return part // splits, pl.ds((part % splits) * (qblocks // splits), qblocks // splits)

    whole = pl.ds(0, qblocks)

    def first_parts(lane):
        if relay and lane == 0:
            return [piece(part) for part in range(2 * splits)]
        return [(kind, whole) for kind in range(2)]

    for lane in range(len(first)):
        for g in range(chunks):
            for kind, rows in first_parts(lane):
                first_copy(lane, g, kind, rows).start()

    def first_wait(lane, g):
        for kind, rows in first_parts(lane):
            first_copy(lane, g, kind, rows).wait_recv()

    slots = []
    for view in views:
        slot = jnp.int32(0)
        for s in range(1, ROLES):
            slot = jnp.where(near_ref[0, s] == view, s, slot)
        slots.append(slot)
    starts = [start_ref[0, slot] for slot in slots]

    def block_of(g):
        cols = slice(g * LANES, (g + 1) * LANES)

        def one_block(b, carry):
            heads = LANES // head_dim
            q = q_ref[b, :, cols] * jnp.asarray(1.0 / math.sqrt(head_dim), jnp.bfloat16)
            lane = lax.broadcasted_iota(jnp.int32, (block_len, LANES), 1) // head_dim
            q2 = jnp.concatenate(
                [jnp.where(lane == h, q, jnp.zeros_like(q)) for h in range(heads)], axis=0
            )
            dims = (((1,), (1,)), ((), ()))
            scores = [
                lax.dot_general(q2, k_ref[b, :, cols], dims, preferred_element_type=jnp.float32)
            ]
            vals = [v_ref[b, :, cols]]
            for r in range(ROLES):
                buffer = buffers[r][g]
                key_parts, val_parts, bias = [], [], []
                live = count_ref[0, slots[r], b]
                for m in range(most):
                    near = starts[r] + block_ref[0, slots[r], b, m]
                    if m > 0:
                        near = jnp.where(m < live, near, 0)
                        bias.append(jnp.where(m < live, 0.0, HIDDEN))
                    key_parts.append(buffer[0, near])
                    val_parts.append(buffer[1, near])
                got = lax.dot_general(
                    q2,
                    jnp.concatenate(key_parts, axis=0),
                    dims,
                    preferred_element_type=jnp.float32,
                )
                pieces = [got[:, :block_len]]
                for m in range(1, most):
                    pieces.append(got[:, m * block_len:(m + 1) * block_len] + bias[m - 1])
                scores.append(jnp.concatenate(pieces, axis=1))
                vals.append(jnp.concatenate(val_parts, axis=0))
            all_scores = jnp.concatenate(scores, axis=1)
            top = jnp.max(all_scores, axis=1, keepdims=True)
            expo = jnp.exp(all_scores - top)
            total = jnp.sum(expo, axis=1, keepdims=True)
            mixed = jnp.dot(
                expo.astype(jnp.bfloat16),
                jnp.concatenate(vals, axis=0),
                preferred_element_type=jnp.float32,
            )
            mixed = mixed / total
            result = mixed[:block_len]
            for h in range(1, heads):
                result = jnp.where(lane == h, mixed[h * block_len:(h + 1) * block_len], result)
            out_ref[b, :, cols] = result.astype(out_ref.dtype)
            return carry

        return one_block

    def compute(g, unroll):
        lax.fori_loop(0, qblocks, block_of(g), 0, unroll=unroll)

    if relay:

        def z_send(g, part):
            return next_copy(part_z, g, part_x, z_to, part)

        def b_send(g, source, part):
            return next_copy(part_b, g, source, partner, part)

        def after_x(g, part):
            first_copy(0, g, *piece(part)).wait_recv()
            z_send(g, part).start()

            @pl.when(from_x)
            def _():
                b_send(g, part_x, part).start()

        def after_z(g, part):
            z_send(g, part).wait_recv()

            @pl.when(jnp.logical_not(from_x))
            def _():
                b_send(g, part_z, part).start()

        def arrive(g):
            first_wait(1, g)

            def one_part(part, carry):
                b_send(g, part_x, part).wait_recv()
                return carry

            lax.fori_loop(0, qblocks, one_part, 0)

        for step in range(chunks + 1):
            if step == 2 or step == chunks < 2:
                for copy in own_copies:
                    copy.wait()
            done = step - 2 if step < chunks else chunks - 2
            if done >= 0:
                arrive(done)

            def one_part(part, carry):
                if step < chunks:
                    after_x(step, part)
                if step >= 1:
                    after_z(step - 1, part)
                if done >= 0:
                    block_of(done)(part, carry)
                return carry

            lax.fori_loop(0, qblocks, one_part, 0)
        arrive(chunks - 1)
        compute(chunks - 1, 3 if qblocks % 3 == 0 else 1)

        for g in range(chunks):

            def one_part(part, carry):
                z_send(g, part).wait_send()

                @pl.when(from_x)
                def _():
                    b_send(g, part_x, part).wait_send()

                @pl.when(jnp.logical_not(from_x))
                def _():
                    b_send(g, part_z, part).wait_send()

                return carry

            lax.fori_loop(0, qblocks, one_part, 0)
    else:
        for copy in own_copies:
            copy.wait()
        for g in range(chunks):
            for lane in range(len(first)):
                first_wait(lane, g)
            compute(g, 1)
    for lane in range(len(first)):
        for g in range(chunks):
            for kind, rows in first_parts(lane):
                first_copy(lane, g, kind, rows).wait_send()


def per_device(
    queries, keys, values, residual, w_out, neighbours, band_start, band_blocks, band_count
):
    tokens, width = queries.shape[1:]
    qblocks = band_count.shape[2]
    most = band_blocks.shape[3]
    cameras = lax.axis_size("cam")
    rigs = cameras // min(32, cameras)
    chunks = width // LANES
    cfg = (cameras, rigs, chunks, qblocks, most, width // HEADS)
    lanes = 2 if relays(cameras, rigs, qblocks) else 4
    dma = pltpu.SemaphoreType.DMA
    anywhere = pl.BlockSpec(memory_space=pl.ANY)
    scalars = pl.BlockSpec(memory_space=pltpu.SMEM)
    blocks = (qblocks, tokens // qblocks, width)
    attended = pl.pallas_call(
        functools.partial(kernel, cfg),
        out_shape=jax.ShapeDtypeStruct(blocks, jnp.bfloat16),
        in_specs=[anywhere] * 3 + [scalars] * 4,
        out_specs=pl.BlockSpec(memory_space=pltpu.VMEM),
        scratch_shapes=[pltpu.VMEM((2,) + blocks[:2] + (LANES,), jnp.bfloat16)] * (ROLES * chunks)
        + [pltpu.VMEM(blocks, jnp.bfloat16)] * 3
        + [
            dma((3,)),
            dma((lanes, chunks, max(2, qblocks))),
            dma((lanes, chunks, max(2, qblocks))),
            dma((2, chunks, qblocks)),
            dma((2, chunks, qblocks)),
        ],
        compiler_params=pltpu.CompilerParams(
            collective_id=0, has_side_effects=True, vmem_limit_bytes=62 * 1024 * 1024
        ),
        name="band_attention",
    )(*(x[0].reshape(blocks) for x in (queries, keys, values)), neighbours, band_start, band_blocks, band_count)
    result = residual[0].astype(jnp.float32) + jnp.dot(
        attended.reshape(tokens, width), w_out, preferred_element_type=jnp.float32
    )
    return result.astype(jnp.bfloat16)[None]


def solution(mesh):
    rows = ("scene", "cam")
    return jax.shard_map(
        per_device,
        mesh=mesh,
        in_specs=(
            P(rows, None, None),
            P(rows, None, None),
            P(rows, None, None),
            P(rows, None, None),
            P(),
            P(rows, None),
            P(rows, None),
            P(rows, None, None, None),
            P(rows, None, None),
        ),
        out_specs=P(rows, None, None),
        check_vma=False,
    )
```
